8 devices in a mesh: parts: 1 (over z), feat: 2 (over y), data: 4 (over x, core).
Axes of the slice: x: 2, y: 2, z: 1, core: 2. Of those that a mesh axis runs over, the one named last changes fastest.
Arguments:
- x_data: bfloat16 [32768, 4096], P('data', 'feat')
- labels: int32 [32768], P('data')
- theta_init: float32 [4096, 128], P('feat', 'parts')
- mom_init: float32 [4096, 128], P('feat', 'parts')
- step_size: float32 [128], P('parts')
Outputs:
- output 1: float32 [4096, 128], P('feat', 'parts')
- output 2: float32 [4096, 128], P('feat', 'parts')
- output 3: float32 [128], P('parts')
All inputs are finite; a program needn't handle non-finite values.
Results may differ from the reference program's by a relative error of at most 0.001.
Values are sent between devices in bfloat16 or wider.
A program may use at most 1 GiB of HBM per device.

```python
import jax
import jax.numpy as jnp
from jax import lax

ROWS = 8192
GROUP = 4
FEATS = 4096
CHAINS = 128
LEAPS = 16
PRIOR_VAR = 4
N_ROWS = ROWS * GROUP


def setup_inputs(seed: int = 0, part: int = 0) -> dict:
    data_key, label_key, mean_key = jax.random.split(jax.random.key(seed), 3)
    chain_key = jax.random.fold_in(jax.random.key(seed + 1), part)
    theta_key, mom_key, spread_key, step_key = jax.random.split(chain_key, 4)
    labels = jax.random.randint(label_key, (N_ROWS,), 0, 2, dtype=jnp.int32)
    sign_vals = (2 * labels - 1).astype(jnp.float32)
    noise_part = jax.random.normal(data_key, (N_ROWS, FEATS), jnp.float32) * FEATS ** -0.5
    class_means = jax.random.normal(mean_key, (GROUP, FEATS), jnp.float32) * (GROUP ** 0.5 / FEATS)
    signal_part = (sign_vals.reshape(GROUP, ROWS, 1) * class_means[:, None, :]).reshape(N_ROWS, FEATS)
    x_data = (noise_part + signal_part).astype(jnp.bfloat16)
    chain_spread = jax.random.uniform(spread_key, (1, CHAINS), jnp.float32, 0.5, 1.5)
    theta_init = jax.random.normal(theta_key, (FEATS, CHAINS), jnp.float32) * chain_spread
    mom_init = jax.random.normal(mom_key, (FEATS, CHAINS), jnp.float32)
    step_size = (0.3 * (FEATS / N_ROWS) ** 0.5) * jax.random.uniform(step_key, (CHAINS,), jnp.float32, 0.75, 1.25)
    return {"x_data": x_data, "labels": labels, "theta_init": theta_init, "mom_init": mom_init, "step_size": step_size}


def reference(x_data, labels, theta_init, mom_init, step_size):
    label_col = labels.astype(jnp.float32)[:, None]

    def gradient_at(position):
        logits = jnp.dot(x_data, position.astype(jnp.bfloat16), preferred_element_type=jnp.float32)
        residual = (label_col - jax.nn.sigmoid(logits)).astype(jnp.bfloat16)
        gradient = jnp.dot(x_data.T, residual, preferred_element_type=jnp.float32)
        return gradient - position / PRIOR_VAR, logits

    half_step = 0.5 * step_size
    gradient, unused_first = gradient_at(theta_init)
    momentum = mom_init + half_step * gradient

    def leap_step(state_pair, unused_in):
        position, momentum = state_pair
        position = position + step_size * momentum
        gradient, unused_out = gradient_at(position)
        return (position, momentum + step_size * gradient), None

    (position, momentum), unused_ys = lax.scan(leap_step, (theta_init, momentum), None, length=LEAPS - 1)
    position = position + step_size * momentum
    gradient, logits = gradient_at(position)
    momentum = momentum + half_step * gradient
    row_loss = jax.nn.softplus(logits) - label_col * logits
    energy = (jnp.sum(row_loss, axis=0) + jnp.sum(position * position, axis=0) / (2 * PRIOR_VAR)
              + 0.5 * jnp.sum(momentum * momentum, axis=0))
    return position, momentum, energy
```

```python
import functools

import jax
import jax.numpy as jnp
from jax import lax
from jax.experimental import pallas as pl
from jax.experimental.pallas import tpu as pltpu
from jax.sharding import PartitionSpec as P

LEAPS = 16
PRIOR_VAR = 4.0
MESH = pl.DeviceIdType.MESH
LANES = 128
F32 = jnp.float32
BF16 = jnp.bfloat16


def contract_last(a, b):
    return lax.dot_general(a, b, (((1,), (1,)), ((), ())), preferred_element_type=F32)


def hmc_kernel(x_hbm, lab_ref, theta_ref, mom_ref, eps_ref,
               th_out, mo_out, en_out,
               xv, zt, rt, gb, dd, hs, rs, tb, tf, pf, eb, ebuf,
               loc_sem, xs_s, xs_r, ds_s, ds_r, rs_s, rs_r, ag_s, ag_r, ad_s, ad_r,
               fx_s, fx_r, fd_s, fd_r, en_s, en_r):
    nb = tb.shape[0]
    chains = zt.shape[1]
    n_zc, z_rows = zt.shape[0], zt.shape[2]
    rows = n_zc * z_rows
    wide = 4 * LANES
    part = lax.axis_index("parts")
    y = lax.axis_index("feat")
    d = lax.axis_index("data")
    x = d // 2
    c = d % 2
    xo, yo, co = 1 - x, 1 - y, 1 - c
    x_nbr = (part, y, 2 * xo + c)
    y_nbr = (part, yo, 2 * x + c)
    diag = (part, yo, 2 * xo + c)
    core = (part, y, 2 * x + co)
    peers = (x_nbr, y_nbr, diag)
    me = 4 * y + d

    def remote(src, dst, s_sem, r_sem, dev):
        return pltpu.make_async_remote_copy(src_ref=src, dst_ref=dst, send_sem=s_sem, recv_sem=r_sem,
                                            device_id=dev, device_id_type=MESH)

    others = []
    for dy in range(2):
        for dd_ in range(4):
            if dy or dd_:
                others.append((part, (y + dy) % 2, (d + dd_) % 4))

    barrier = pltpu.get_barrier_semaphore()
    for dev in others:
        pl.semaphore_signal(barrier, inc=1, device_id=dev, device_id_type=MESH)
    pl.semaphore_wait(barrier, 7)

    def x_copy(i):
        n = rows // xs_s.shape[0]
        return remote(x_hbm.at[pl.ds(pl.multiple_of(yo * rows + i * n, n), n), :],
                      xv.at[y, pl.ds(pl.multiple_of(i * n, n), n), :], xs_s.at[i], xs_r.at[i], y_nbr)

    def d2d_copy(j):
        return remote(gb.at[j, co], dd.at[j], ds_s.at[j], ds_r.at[j], core)

    def rs_copy(j, k):
        src = (hs.at[j, y, xo], hs.at[j, yo, x], hs.at[j, yo, xo])[k]
        return remote(src, rs.at[j, k], rs_s.at[j, k], rs_r.at[j, k], peers[k])

    def ag_copy(j, k):
        return remote(tb.at[j, c, y, x], tb.at[j, c, y, x], ag_s.at[j, k], ag_r.at[j, k], peers[k])

    def agd_copy(j):
        return remote(tb.at[j, c], tb.at[j, c], ad_s.at[j], ad_r.at[j], core)

    eb[...] = jnp.broadcast_to(eps_ref[...], (LANES, chains)).T
    for j in range(nb):
        tile = theta_ref[j, c, x].T
        tf[j] = tile
        tb[j, c, y, x] = tile.astype(BF16)
        pf[j] = mom_ref[j, c, x].T
        for k in range(3):
            ag_copy(j, k).start()
    n_x = xs_s.shape[0]

    @pl.loop(0, n_x)
    def _(i):
        x_copy(i).start()

    local = pltpu.make_async_copy(x_hbm.at[pl.ds(pl.multiple_of(y * rows, rows), rows), :], xv.at[y], loc_sem)
    local.start()

    def gather_mid(j):
        for k in range(3):
            ag_copy(j, k).wait()
        agd_copy(j).start()

    def gather_end(j):
        agd_copy(j).wait()

    for j in range(nb):
        gather_mid(j)
    for j in range(nb):
        gather_end(j)
    local.wait()

    def lhs_of(j, h):
        return jnp.concatenate([tb[j, cc, h, xx] for cc in range(2) for xx in range(2)], axis=1)

    def residual(i, z):
        lab = lab_ref[:, pl.ds(pl.multiple_of(y * rows + i * z_rows, z_rows), z_rows)]
        rt[:, pl.ds(pl.multiple_of(i * z_rows, z_rows), z_rows)] = (lab - jax.nn.sigmoid(z)).astype(BF16)

    @pl.loop(0, n_x)
    def _(i):
        x_copy(i).wait_recv()
        n = rows // n_x
        at = pl.ds(pl.multiple_of(i * n, n), n)
        acc = jnp.zeros((chains, n), F32)
        for j in range(nb):
            for h in range(2):
                acc = acc + contract_last(lhs_of(j, h), xv[h, at, j * wide:(j + 1) * wide])
        lab = lab_ref[:, pl.ds(pl.multiple_of(y * rows + i * n, n), n)]
        rt[:, at] = (lab - jax.nn.sigmoid(acc)).astype(BF16)

    @pl.loop(0, n_x)
    def _(i):
        x_copy(i).wait_send()

    def grad_block(j):
        cols = pl.ds(pl.multiple_of(j * wide, wide), wide)
        for h in range(2):
            out = jnp.dot(rt[...], xv[h, :, cols], preferred_element_type=F32)
            for cc in range(2):
                for xx in range(2):
                    k = 2 * cc + xx
                    gb[j, cc, h, xx] = out[:, k * LANES:(k + 1) * LANES]
        d2d_copy(j).start()

    def pair_sum(j):
        d2d_copy(j).wait()
        hs[j] = gb[j, c] + dd[j]
        for k in range(3):
            rs_copy(j, k).start()

    def update(j, t):
        for k in range(3):
            rs_copy(j, k).wait()
        total = (hs[j, y, x] + rs[j, 0]) + (rs[j, 1] + rs[j, 2])
        pos = tf[j]
        ends = jnp.logical_or(t == 0, t == LEAPS)
        scale = eb[...] * jnp.where(ends, 0.5, 1.0)
        mom = pf[j] + scale * (total - pos / PRIOR_VAR)
        pf[j] = mom

        @pl.when(t < LEAPS)
        def _():
            new = pos + eb[...] * mom
            tf[j] = new
            tb[j, c, y, x] = new.astype(BF16)
            for k in range(3):
                ag_copy(j, k).start()

    def logits_block(j):
        cols = pl.ds(pl.multiple_of(j * wide, wide), wide)
        left = [lhs_of(j, h) for h in range(2)]

        @pl.loop(0, n_zc)
        def _(i):
            at = pl.ds(pl.multiple_of(i * z_rows, z_rows), z_rows)
            new = contract_last(left[0], xv[0, at, cols]) + contract_last(left[1], xv[1, at, cols])
            zt[i] = jnp.where(j == 0, 0.0, zt[i]) + new

    d_mid, d_upd, d_gat, d_log = 1, 3, 4, 5

    def one_eval(t, carry):
        steps = jnp.where(t < LEAPS, nb + d_log, nb + d_upd)

        def step(s, carry):
            def on(delay, fn, *args):
                @pl.when(jnp.logical_and(s >= delay, s < nb + delay))
                def _():
                    fn(s - delay, *args)

            on(0, grad_block)
            on(d_mid, pair_sum)
            on(d_upd, update, t)

            @pl.when(t < LEAPS)
            def _():
                on(d_gat, gather_mid)

                @pl.when(jnp.logical_and(s >= d_log, s < nb + d_log))
                def _():
                    gather_end(s - d_log)
                    logits_block(s - d_log)

                @pl.when(s == nb + d_log - 1)
                def _():
                    @pl.loop(0, n_zc)
                    def _(i):
                        residual(i, zt[i])
            return carry

        return lax.fori_loop(0, steps, step, carry)

    lax.fori_loop(0, LEAPS + 1, one_eval, 0)

    for j in range(nb):
        th_out[j, c, x] = tf[j].T
        mo_out[j, c, x] = pf[j].T
    outs = (th_out, mo_out)
    fx = [remote(o.at[:, c, x], o.at[:, c, x], fx_s.at[n], fx_r.at[n], x_nbr) for n, o in enumerate(outs)]
    for cp in fx:
        cp.start()

    def loss(i, acc):
        z = zt[i]
        lab = lab_ref[:, pl.ds(pl.multiple_of(y * rows + i * z_rows, z_rows), z_rows)]
        soft = jnp.maximum(z, 0.0) + jnp.log1p(jnp.exp(-jnp.abs(z)))
        term = soft - lab * z
        for q in range(z_rows // LANES):
            acc = acc + term[:, q * LANES:(q + 1) * LANES]
        return acc

    acc = lax.fori_loop(0, n_zc, loss, jnp.zeros((chains, LANES), F32))
    for j in range(nb):
        acc = acc + tf[j] * tf[j] * (1.0 / (2.0 * PRIOR_VAR)) + 0.5 * (pf[j] * pf[j])
    row = jnp.sum(acc.T, axis=0, keepdims=True)
    ebuf[me] = jnp.broadcast_to(row, (8, chains))
    sends = []
    for n, dev in enumerate(others):
        cp = remote(ebuf.at[me], ebuf.at[me], en_s.at[n], en_r.at[n], dev)
        cp.start()
        sends.append(cp)

    for cp in fx:
        cp.wait()
    fd = [remote(o.at[:, c], o.at[:, c], fd_s.at[n], fd_r.at[n], core) for n, o in enumerate(outs)]
    for cp in fd:
        cp.start()
    for cp in sends:
        cp.wait()
    total = ebuf[0]
    for n in range(1, 8):
        total = total + ebuf[n]
    en_out[...] = total[0:1]
    for cp in fd:
        cp.wait()


def solution(mesh):
    chain_spec = P("feat", "parts")

    def local_run(x_local, labels, theta_init, mom_init, step_size):
        n_local, feats_half = x_local.shape
        rows = n_local // 2
        chains = theta_init.shape[1]
        nb = feats_half // (4 * LANES)
        z_rows = min(4096, rows)
        n_x = 16
        tiles = (nb, 2, 2, LANES, chains)
        vm = pl.BlockSpec(memory_space=pltpu.VMEM)
        dma = pltpu.SemaphoreType.DMA
        th, mo, en = pl.pallas_call(
            hmc_kernel,
            out_shape=(jax.ShapeDtypeStruct(tiles, F32), jax.ShapeDtypeStruct(tiles, F32),
                       jax.ShapeDtypeStruct((1, chains), F32)),
            in_specs=[pl.BlockSpec(memory_space=pl.ANY), vm, vm, vm, vm],
            out_specs=(vm, vm, vm),
            scratch_shapes=[
                pltpu.VMEM((2, rows, feats_half), BF16),
                pltpu.VMEM((rows // z_rows, chains, z_rows), F32),
                pltpu.VMEM((chains, rows), BF16),
                pltpu.VMEM((nb, 2, 2, 2, chains, LANES), F32),
                pltpu.VMEM((nb, 2, 2, chains, LANES), F32),
                pltpu.VMEM((nb, 2, 2, chains, LANES), F32),
                pltpu.VMEM((nb, 3, chains, LANES), F32),
                pltpu.VMEM((nb, 2, 2, 2, chains, LANES), BF16),
                pltpu.VMEM((nb, chains, LANES), F32),
                pltpu.VMEM((nb, chains, LANES), F32),
                pltpu.VMEM((chains, LANES), F32),
                pltpu.VMEM((8, 8, chains), F32),
                dma, dma((n_x,)), dma((n_x,)), dma((nb,)), dma((nb,)), dma((nb, 3)), dma((nb, 3)),
                dma((nb, 3)), dma((nb, 3)), dma((nb,)), dma((nb,)),
                dma((2,)), dma((2,)), dma((2,)), dma((2,)), dma((7,)), dma((7,)),
            ],
            compiler_params=pltpu.CompilerParams(collective_id=0, has_side_effects=True,
                                                 vmem_limit_bytes=62 * 1024 * 1024),
        )(x_local, labels.astype(F32)[None, :], theta_init.reshape(tiles), mom_init.reshape(tiles),
          step_size[None, :])
        return th.reshape(theta_init.shape), mo.reshape(theta_init.shape), en.reshape(chains)

    return jax.shard_map(local_run, mesh=mesh,
                         in_specs=(P("data", "feat"), P("data"), chain_spec, chain_spec, P("parts")),
                         out_specs=(chain_spec, chain_spec, P("parts")), check_vma=False)
```

```python
import functools

import jax
import jax.numpy as jnp
from jax import lax
from jax.experimental import pallas as pl
from jax.experimental.pallas import tpu as pltpu
from jax.sharding import PartitionSpec as P

LEAPS = 16
PRIOR_VAR = 4.0
MESH = pl.DeviceIdType.MESH
LANES = 128
F32 = jnp.float32
BF16 = jnp.bfloat16


def contract_last(a, b):
    return lax.dot_general(a, b, (((1,), (1,)), ((), ())), preferred_element_type=F32)


def hmc_kernel(x_hbm, lab_ref, theta_ref, mom_ref, eps_ref,
               th_out, mo_out, en_out,
               xv, xw, zt, rt, gb, dd, r1, h2, r2, tb, tf, pf, xt, eb, lsum, ebuf,
               loc_sem, io_sem, xs_s, xs_r, in_s, in_r, ds_s, ds_r, r1_s, r1_r, r2_s, r2_r, a1_s, a1_r, ad_s, ad_r,
               fx_s, fx_r, fd_s, fd_r, en_s, en_r):
    nb = tb.shape[0]
    chains = zt.shape[1]
    n_zc, z_rows = zt.shape[0], zt.shape[2]
    rows = n_zc * z_rows
    wide = 4 * LANES
    part = lax.axis_index("parts")
    y = lax.axis_index("feat")
    d = lax.axis_index("data")
    x = d // 2
    c = d % 2
    xo, yo, co = 1 - x, 1 - y, 1 - c
    x_nbr = (part, y, 2 * xo + c)
    y_nbr = (part, yo, 2 * x + c)
    core = (part, y, 2 * x + co)
    pair = (x_nbr, y_nbr)
    half = chains // 2
    me = 4 * y + d

    def remote(src, dst, s_sem, r_sem, dev):
        return pltpu.make_async_remote_copy(src_ref=src, dst_ref=dst, send_sem=s_sem, recv_sem=r_sem,
                                            device_id=dev, device_id_type=MESH)

    others = []
    for dy in range(2):
        for dd_ in range(4):
            if dy or dd_:
                others.append((part, (y + dy) % 2, (d + dd_) % 4))

    barrier = pltpu.get_barrier_semaphore()
    for dev in others:
        pl.semaphore_signal(barrier, inc=1, device_id=dev, device_id_type=MESH)
    pl.semaphore_wait(barrier, 7)

    def x_copy(i):
        n = rows // xs_s.shape[0]
        return remote(x_hbm.at[pl.ds(pl.multiple_of(yo * rows + i * n, n), n), :],
                      xv.at[y, pl.ds(pl.multiple_of(i * n, n), n), :], xs_s.at[i], xs_r.at[i], y_nbr)

    def d2d_copy(j):
        return remote(gb.at[j, co], dd.at[j], ds_s.at[j], ds_r.at[j], core)

    def rs1_copy(j, k):
        src = (gb.at[j, c, :, xo, :half], gb.at[j, c, yo, :, half:])[k]
        return remote(src, r1.at[j, k], r1_s.at[j, k], r1_r.at[j, k], pair[k])

    def rs2_copy(j, k):
        return remote(h2.at[j, k], r2.at[j, k], r2_s.at[j, k], r2_r.at[j, k], pair[1 - k])

    def ag1_copy(j, k):
        ref = (tb.at[j, c, 0, :, x], tb.at[j, c, 1, y])[k]
        return remote(ref, ref, a1_s.at[j, k], a1_r.at[j, k], pair[k])

    def start_copy(n):
        ref = (tf, pf)[n].at[:, 0, y]
        return remote(ref, ref, in_s.at[n], in_r.at[n], y_nbr)

    def last_copy(n):
        return remote((tf, pf)[n].at[:, 0, y], xt.at[n], fx_s.at[n], fx_r.at[n], x_nbr)

    def agd_copy(j):
        return remote(tb.at[j, c], tb.at[j, c], ad_s.at[j], ad_r.at[j], core)

    n_x = xs_s.shape[0]
    ahead = 2
    staged = [pltpu.make_async_copy(ref.at[:, c], gb.at[:, n, c], io_sem.at[n])
              for n, ref in enumerate((theta_ref, mom_ref))]
    for cp in staged:
        cp.start()
    for i in range(ahead):
        x_copy(i).start()
    local = pltpu.make_async_copy(x_hbm.at[pl.ds(pl.multiple_of(y * rows, rows), rows), :], xv.at[y], loc_sem)
    local.start()
    eb[...] = jnp.broadcast_to(eps_ref[...], (LANES, chains)).T
    for cp in staged:
        cp.wait()
    for j in range(nb):
        for xx in range(2):
            tf[j, 1, xx] = gb[j, 0, c, xx].T[half:]
            pf[j, 1, xx] = gb[j, 1, c, xx].T[half:]
            tb[j, c, 1, y, xx] = tf[j, 1, xx].astype(BF16)
        tf[j, 0, y] = gb[j, 0, c, x].T[:half]
        pf[j, 0, y] = gb[j, 1, c, x].T[:half]
    start_copy(0).start()
    for j in range(nb):
        ag1_copy(j, 1).start()

    @pl.loop(ahead, n_x)
    def _(i):
        x_copy(i).start()

    start_copy(1).start()

    def gather_mid(j):
        for k in range(2):
            ag1_copy(j, k).wait()
        agd_copy(j).start()

    def gather_end(j):
        agd_copy(j).wait()

    start_copy(0).wait()
    for j in range(nb):
        tb[j, c, 0, :, x] = tf[j, 0].astype(BF16)
        ag1_copy(j, 0).start()
    for j in range(nb):
        gather_mid(j)
    for j in range(nb):
        gather_end(j)
    local.wait()

    def lhs_of(j, h):
        top = jnp.concatenate([tb[j, cc, 0, h, xx] for cc in range(2) for xx in range(2)], axis=1)
        low = jnp.concatenate([tb[j, cc, 1, h, xx] for cc in range(2) for xx in range(2)], axis=1)
        return jnp.concatenate([top, low], axis=0)

    def label_row(i, n):
        return lab_ref[:, pl.ds(pl.multiple_of(y * rows + i * n, n), n)].astype(F32)

    def residual(i, z):
        lab = label_row(i, z_rows)
        rt[:, pl.ds(pl.multiple_of(i * z_rows, z_rows), z_rows)] = (lab - jax.nn.sigmoid(z)).astype(BF16)

    @pl.loop(0, n_x)
    def _(i):
        x_copy(i).wait_recv()
        n = rows // n_x
        at = pl.ds(pl.multiple_of(i * n, n), n)
        acc = jnp.zeros((chains, n), F32)
        for j in range(nb):
            for h in range(2):
                acc = acc + contract_last(lhs_of(j, h), xv[h, at, j * wide:(j + 1) * wide])
        lab = label_row(i, n)
        rt[:, at] = (lab - jax.nn.sigmoid(acc)).astype(BF16)
        for j in range(xw.shape[0]):
            for h in range(2):
                src = (nb - xw.shape[0] + j) * wide
                xw[j, h * wide:(h + 1) * wide, at] = xv[h, at, src:src + wide].T

    @pl.loop(0, n_x)
    def _(i):
        x_copy(i).wait_send()

    start_copy(1).wait()

    def grad_block(j):
        cols = pl.ds(pl.multiple_of(j * wide, wide), wide)
        for h in range(2):
            out = jnp.dot(rt[...], xv[h, :, cols], preferred_element_type=F32)
            for q in range(4):
                gb[j, q // 2, h, q % 2] = out[:, q * LANES:(q + 1) * LANES]
        d2d_copy(j).start()

    def pair_sum(j):
        d2d_copy(j).wait()
        gb[j, c] += dd[j]
        for k in range(2):
            rs1_copy(j, k).start()

    def chip_sum(j):
        for k in range(2):
            rs1_copy(j, k).wait()
        h2[j, 0] = gb[j, c, :, x, :half] + r1[j, 0]
        h2[j, 1] = gb[j, c, y, :, half:] + r1[j, 1]
        for k in range(2):
            rs2_copy(j, k).start()

    def update(j, t):
        for k in range(2):
            rs2_copy(j, k).wait()
        pos = tf[j]
        eps = eb[...].reshape(2, 1, half, LANES)
        ends = jnp.logical_or(t == 0, t == LEAPS)
        mom = pf[j] + eps * jnp.where(ends, 0.5, 1.0) * ((h2[j] + r2[j]) - pos / PRIOR_VAR)
        pf[j] = mom

        @pl.when(t < LEAPS)
        def _():
            new = pos + eps * mom
            tf[j] = new
            low = new.astype(BF16)
            tb[j, c, 0, :, x] = low[0]
            tb[j, c, 1, y] = low[1]
            for k in range(2):
                ag1_copy(j, k).start()

    n_slow = nb - xw.shape[0]

    def logits_block(j):
        left = [lhs_of(j, h) for h in range(2)]

        @pl.when(j < n_slow)
        def _():
            cols = pl.ds(pl.multiple_of(j * wide, wide), wide)

            @pl.loop(0, n_zc)
            def _(i):
                at = pl.ds(pl.multiple_of(i * z_rows, z_rows), z_rows)
                new = contract_last(left[0], xv[0, at, cols]) + contract_last(left[1], xv[1, at, cols])
                zt[i] = jnp.where(j == 0, 0.0, zt[i]) + new

        @pl.when(j >= n_slow)
        def _():
            both = jnp.concatenate(left, axis=1)

            @pl.loop(0, n_zc)
            def _(i):
                at = pl.ds(pl.multiple_of(i * z_rows, z_rows), z_rows)
                zt[i] += jnp.dot(both, xw[j - n_slow, :, at], preferred_element_type=F32)

    d_mid, d_chp, d_upd, d_gat, d_log = 1, 3, 4, 5, 6

    def loss(i, acc):
        z = zt[i]
        soft = jnp.maximum(z, 0.0) + jnp.log1p(jnp.exp(-jnp.abs(z)))
        term = soft - label_row(i, z_rows) * z
        for q in range(z_rows // LANES):
            acc = acc + term[:, q * LANES:(q + 1) * LANES]
        return acc

    def one_eval(t, carry):
        steps = jnp.where(t < LEAPS, nb + d_log, nb + d_upd)

        def step(s, carry):
            def on(delay, fn, *args):
                @pl.when(jnp.logical_and(s >= delay, s < nb + delay))
                def _():
                    fn(s - delay, *args)

            @pl.when(jnp.logical_and(t == LEAPS, s == 0))
            def _():
                last_copy(0).start()

            @pl.when(jnp.logical_and(t == LEAPS, s == nb))
            def _():
                lsum[...] = lax.fori_loop(0, n_zc, loss, jnp.zeros((chains, LANES), F32))

            on(0, grad_block)
            on(d_mid, pair_sum)
            on(d_chp, chip_sum)
            on(d_upd, update, t)

            @pl.when(t < LEAPS)
            def _():
                on(d_gat, gather_mid)

                @pl.when(jnp.logical_and(s >= d_log, s < nb + d_log))
                def _():
                    gather_end(s - d_log)
                    logits_block(s - d_log)

                @pl.when(s == nb + d_log - 1)
                def _():
                    @pl.loop(0, n_zc)
                    def _(i):
                        residual(i, zt[i])
            return carry

        return lax.fori_loop(0, steps, step, carry)

    lax.fori_loop(0, LEAPS + 1, one_eval, 0)

    last_copy(1).start()
    acc = lsum[...]
    for j in range(nb):
        for h in range(2):
            own = tf[j, 0, h] * tf[j, 0, h] * (1.0 / (2.0 * PRIOR_VAR)) + 0.5 * (pf[j, 0, h] * pf[j, 0, h])
            twin = tf[j, 1, h] * tf[j, 1, h] * (1.0 / (2.0 * PRIOR_VAR)) + 0.5 * (pf[j, 1, h] * pf[j, 1, h])
            acc = acc + jnp.concatenate([jnp.where(h == y, own, 0.0), jnp.where(h == x, twin, 0.0)], axis=0)
    row = jnp.sum(acc.T, axis=0, keepdims=True)
    ebuf[me] = jnp.broadcast_to(row, (8, chains))
    sends = []
    for n, dev in enumerate(others):
        cp = remote(ebuf.at[me], ebuf.at[me], en_s.at[n], en_r.at[n], dev)
        cp.start()
        sends.append(cp)

    for cp in sends:
        cp.wait()
    total = ebuf[0]
    for n in range(1, 8):
        total = total + ebuf[n]
    en_out[...] = total[0:1]

    def put(n, k):
        cc = (c, co)[k]
        return pltpu.make_async_copy(gb.at[:, n, cc], (th_out, mo_out)[n].at[:, cc], io_sem.at[2 * k + n])

    def swap(n):
        return remote(gb.at[:, n, c], gb.at[:, n, c], fd_s.at[n], fd_r.at[n], core)

    for n in range(2):
        last_copy(n).wait()
        state = (tf, pf)[n]
        for j in range(nb):
            gb[j, n, c, x] = jnp.concatenate([state[j, 0, y], state[j, 1, x]], axis=0).T
            gb[j, n, c, xo] = jnp.concatenate([xt[n, j], state[j, 1, xo]], axis=0).T
        swap(n).start()
        put(n, 0).start()
    for n in range(2):
        swap(n).wait()
        put(n, 1).start()
    for n in range(2):
        put(n, 0).wait()
        put(n, 1).wait()


def solution(mesh):
    chain_spec = P("feat", "parts")

    def local_run(x_local, labels, theta_init, mom_init, step_size):
        n_local, feats_half = x_local.shape
        rows = n_local // 2
        chains = theta_init.shape[1]
        nb = feats_half // (4 * LANES)
        z_rows = min(4096, rows)
        n_x = 16
        tiles = (nb, 2, 2, LANES, chains)
        vm = pl.BlockSpec(memory_space=pltpu.VMEM)
        dma = pltpu.SemaphoreType.DMA
        far = pl.BlockSpec(memory_space=pl.ANY)
        th, mo, en = pl.pallas_call(
            hmc_kernel,
            out_shape=(jax.ShapeDtypeStruct(tiles, F32), jax.ShapeDtypeStruct(tiles, F32),
                       jax.ShapeDtypeStruct((1, chains), F32)),
            in_specs=[far, vm, far, far, vm],
            out_specs=(far, far, vm),
            scratch_shapes=[
                pltpu.VMEM((2, rows, feats_half), BF16),
                pltpu.VMEM((nb // 2, 8 * LANES, rows), BF16),
                pltpu.VMEM((rows // z_rows, chains, z_rows), F32),
                pltpu.VMEM((chains, rows), BF16),
                pltpu.VMEM((nb, 2, 2, 2, chains, LANES), F32),
                pltpu.VMEM((nb, 2, 2, chains, LANES), F32),
                pltpu.VMEM((nb, 2, 2, chains // 2, LANES), F32),
                pltpu.VMEM((nb, 2, 2, chains // 2, LANES), F32),
                pltpu.VMEM((nb, 2, 2, chains // 2, LANES), F32),
                pltpu.VMEM((nb, 2, 2, 2, 2, chains // 2, LANES), BF16),
                pltpu.VMEM((nb, 2, 2, chains // 2, LANES), F32),
                pltpu.VMEM((nb, 2, 2, chains // 2, LANES), F32),
                pltpu.VMEM((2, nb, chains // 2, LANES), F32),
                pltpu.VMEM((chains, LANES), F32),
                pltpu.VMEM((chains, LANES), F32),
                pltpu.VMEM((8, 8, chains), F32),
                dma, dma((4,)), dma((n_x,)), dma((n_x,)), dma((2,)), dma((2,)), dma((nb,)), dma((nb,)),
                dma((nb, 2)), dma((nb, 2)), dma((nb, 2)), dma((nb, 2)),
                dma((nb, 2)), dma((nb, 2)), dma((nb,)), dma((nb,)),
                dma((2,)), dma((2,)), dma((2,)), dma((2,)), dma((7,)), dma((7,)),
            ],
            compiler_params=pltpu.CompilerParams(collective_id=0, has_side_effects=True,
                                                 vmem_limit_bytes=67043328),
        )(x_local, labels[None, :], theta_init.reshape(tiles), mom_init.reshape(tiles),
          step_size[None, :])
        return th.reshape(theta_init.shape), mo.reshape(theta_init.shape), en.reshape(chains)

    return jax.shard_map(local_run, mesh=mesh,
                         in_specs=(P("data", "feat"), P("data"), chain_spec, chain_spec, P("parts")),
                         out_specs=(chain_spec, chain_spec, P("parts")), check_vma=False)
```

```python
import functools

import jax
import jax.numpy as jnp
from jax import lax
from jax.experimental import pallas as pl
from jax.experimental.pallas import tpu as pltpu
from jax.sharding import PartitionSpec as P

LEAPS = 16
PRIOR_VAR = 4.0
MESH = pl.DeviceIdType.MESH
LANES = 128
PLAN = (
        "e0", "g0", "h0", "g1", "p0", "h1", "g2", "p1", "h2", "p2", "c0", "g3",
        "c1", "h3", "p3", "l0", "u0", "c2", "c3", "u1", "m0", "o0", "u2", "t0",
        "u3", "m1", "o1", "m2", "o2", "t1", "m3", "o3", "t2", "t3",
)
F32 = jnp.float32
BF16 = jnp.bfloat16


def contract_last(a, b):
    return lax.dot_general(a, b, (((1,), (1,)), ((), ())), preferred_element_type=F32)


def hmc_kernel(x_hbm, lab_ref, theta_ref, mom_ref, eps_ref,
               th_out, mo_out, en_out,
               xa, zt, rt, gb, dd, r1, h2, r2, tb, tf, pf, xt, eb, lsum, ebuf,
               loc_sem, io_sem, xs_s, xs_r, in_s, in_r, ds_s, ds_r, r1_s, r1_r, r2_s, r2_r, a1_s, a1_r, ad_s, ad_r,
               fx_s, fx_r, fd_s, fd_r, en_s, en_r):
    nb = tb.shape[0]
    chains = zt.shape[1]
    n_zc, z_rows = zt.shape[0], zt.shape[2]
    rows = n_zc * z_rows
    wide = 4 * LANES
    strip = 2 * LANES
    n_x = 2 * nb
    part = lax.axis_index("parts")
    y = lax.axis_index("feat")
    d = lax.axis_index("data")
    x = d // 2
    c = d % 2
    xo, yo, co = 1 - x, 1 - y, 1 - c
    x_nbr = (part, y, 2 * xo + c)
    y_nbr = (part, yo, 2 * x + c)
    core = (part, y, 2 * x + co)
    pair = (x_nbr, y_nbr)
    half = chains // 2
    me = 4 * y + d

    def remote(src, dst, s_sem, r_sem, dev):
        return pltpu.make_async_remote_copy(src_ref=src, dst_ref=dst, send_sem=s_sem, recv_sem=r_sem,
                                            device_id=dev, device_id_type=MESH)

    others = []
    for dy in range(2):
        for dd_ in range(4):
            if dy or dd_:
                others.append((part, (y + dy) % 2, (d + dd_) % 4))

    barrier = pltpu.get_barrier_semaphore()
    for dev in others:
        pl.semaphore_signal(barrier, inc=1, device_id=dev, device_id_type=MESH)
    pl.semaphore_wait(barrier, 7)

    def strip_refs(u, here):
        src = x_hbm.at[pl.ds(pl.multiple_of(here * rows, rows), rows), pl.ds(pl.multiple_of(u * strip, strip), strip)]
        return src, xa.at[u, :, pl.ds(pl.multiple_of(y * strip, strip), strip)]

    def x_copy(u):
        return remote(*strip_refs(u, yo), xs_s.at[u], xs_r.at[u], y_nbr)

    def x_local(u):
        return pltpu.make_async_copy(*strip_refs(u, y), loc_sem.at[u])

    def d2d_copy(j):
        return remote(gb.at[j, co], dd.at[j], ds_s.at[j], ds_r.at[j], core)

    def rs1_copy(j, k):
        src = (gb.at[j, c, :, xo, :half], gb.at[j, c, yo, :, half:])[k]
        return remote(src, r1.at[j, k], r1_s.at[j, k], r1_r.at[j, k], pair[k])

    def rs2_copy(j, k):
        return remote(h2.at[j, k], r2.at[j, k], r2_s.at[j, k], r2_r.at[j, k], pair[1 - k])

    def ag1_copy(j, k):
        ref = (tb.at[j, c, 0, :, x], tb.at[j, c, 1, y])[k]
        return remote(ref, ref, a1_s.at[j, k], a1_r.at[j, k], pair[k])

    def start_copy(n):
        ref = (tf, pf)[n].at[:, 0, y]
        return remote(ref, ref, in_s.at[n], in_r.at[n], y_nbr)

    def last_copy(n, j):
        return remote((tf, pf)[n].at[j, 0, y], xt.at[n, j], fx_s.at[n, j], fx_r.at[n, j], x_nbr)

    def agd_copy(j):
        return remote(tb.at[j, c], tb.at[j, c], ad_s.at[j], ad_r.at[j], core)

    ahead = 1

    def strip_at(i):
        return n_x - 2 - 2 * (i // 2) + i % 2

    staged = [pltpu.make_async_copy(ref.at[:, c], gb.at[:, n, c], io_sem.at[n])
              for n, ref in enumerate((theta_ref, mom_ref))]
    for cp in staged:
        cp.start()
    for i in range(ahead):
        x_copy(strip_at(i)).start()
    for i in range(n_x):
        x_local(strip_at(i)).start()
    eb[...] = jnp.broadcast_to(eps_ref[...], (LANES, chains)).T
    for cp in staged:
        cp.wait()
    for j in range(nb):
        for xx in range(2):
            tf[j, 1, xx] = gb[j, 0, c, xx].T[half:]
            pf[j, 1, xx] = gb[j, 1, c, xx].T[half:]
            tb[j, c, 1, y, xx] = tf[j, 1, xx].astype(BF16)
        tf[j, 0, y] = gb[j, 0, c, x].T[:half]
        pf[j, 0, y] = gb[j, 1, c, x].T[:half]
    start_copy(0).start()
    for j in range(nb):
        ag1_copy(j, 1).start()

    @pl.loop(ahead, n_x)
    def _(i):
        x_copy(strip_at(i)).start()

    start_copy(1).start()

    def gather_mid(j):
        for k in range(2):
            ag1_copy(j, k).wait()
        agd_copy(j).start()

    def gather_end(j):
        agd_copy(j).wait()

    start_copy(0).wait()
    for j in range(nb):
        tb[j, c, 0, :, x] = tf[j, 0].astype(BF16)
        ag1_copy(j, 0).start()
    for j in range(nb):
        gather_mid(j)
    for j in range(nb):
        gather_end(j)

    def lhs_of(j, cc):
        return jnp.concatenate([jnp.concatenate([tb[j, cc, k, h, xx] for h in range(2) for xx in range(2)], axis=1)
                                for k in range(2)], axis=0)

    def label_row(i, n):
        return lab_ref[:, pl.ds(pl.multiple_of(y * rows + i * n, n), n)].astype(F32)

    def residual(i, z):
        lab = label_row(i, z_rows)
        rt[:, pl.ds(pl.multiple_of(i * z_rows, z_rows), z_rows)] = (lab - jax.nn.sigmoid(z)).astype(BF16)

    def piece(q):
        return slice(q * z_rows, (q + 1) * z_rows)

    def logits_plain(j, cc, first):
        left = lhs_of(j, cc)
        for q in range(n_zc):
            new = contract_last(left, xa[2 * j + cc, piece(q)])
            zt[q] = new if first is True else jnp.where(first, 0.0, zt[q]) + new

    def logits_flip(j, cc, end):
        left = lhs_of(j, cc)
        for q in range(n_zc):
            z = zt[q] + jnp.dot(left, xa[nb + 2 * j + cc, piece(q)], preferred_element_type=F32)
            zt[q] = z
            if end:
                residual(q, z)

    @pl.loop(0, n_x)
    def _(i):
        u = strip_at(i)
        j, cc = u // 2, u % 2
        x_local(u).wait()
        x_copy(u).wait_recv()
        logits_plain(j, cc, i == 0)

        @pl.when(j > 0)
        def _():
            for q in range(n_zc):
                xa[nb + u, piece(q)] = xa[u, piece(q)].T

    for q in range(n_zc):
        residual(q, zt[q])

    @pl.loop(0, n_x)
    def _(i):
        x_copy(i).wait_send()

    start_copy(1).wait()

    def grad_half(j, p):
        if j < nb - 1:
            out = jnp.dot(rt[...], xa[2 * j + p], preferred_element_type=F32)
        else:
            out = contract_last(rt[:, piece(0)], xa[nb + 2 * j + p, piece(0)])
            for q in range(1, n_zc):
                out = out + contract_last(rt[:, piece(q)], xa[nb + 2 * j + p, piece(q)])
        for q in range(4):
            gb[j, p, q // 2, q % 2] = out[:, q * LANES:(q + 1) * LANES]

    def grad_twin(j, t):
        grad_half(j, co)
        d2d_copy(j).start()

    def grad_own(j, t):
        grad_half(j, c)

    def pair_sum(j, t):
        d2d_copy(j).wait()
        gb[j, c] += dd[j]
        for k in range(2):
            rs1_copy(j, k).start()

    def chip_sum(j, t):
        for k in range(2):
            rs1_copy(j, k).wait()
        h2[j, 0] = gb[j, c, :, x, :half] + r1[j, 0]
        h2[j, 1] = gb[j, c, y, :, half:] + r1[j, 1]
        for k in range(2):
            rs2_copy(j, k).start()

    def update(j, t):
        for k in range(2):
            rs2_copy(j, k).wait()
        pos = tf[j]
        eps = eb[...].reshape(2, 1, half, LANES)
        ends = jnp.logical_or(t == 0, t == LEAPS)
        mom = pf[j] + eps * jnp.where(ends, 0.5, 1.0) * ((h2[j] + r2[j]) - pos / PRIOR_VAR)
        pf[j] = mom

        @pl.when(t < LEAPS)
        def _():
            new = pos + eps * mom
            tf[j] = new
            low = new.astype(BF16)
            tb[j, c, 0, :, x] = low[0]
            tb[j, c, 1, y] = low[1]
            for k in range(2):
                ag1_copy(j, k).start()

        @pl.when(t == LEAPS)
        def _():
            last_copy(1, j).start()

    def logits_own(j, t):
        if j == 0:
            logits_plain(j, c, True)
        else:
            logits_flip(j, c, False)

    def logits_twin(j, t):
        gather_end(j)
        if j == 0:
            logits_plain(j, co, False)
        else:
            logits_flip(j, co, j == nb - 1)

    def gather(j, t):
        gather_mid(j)

    def first_end(j, t):
        @pl.when(t == LEAPS)
        def _():
            for i in range(nb):
                last_copy(0, i).start()

    def add_loss(j, t):
        @pl.when(t == LEAPS)
        def _():
            lsum[...] = lax.fori_loop(0, n_zc, loss, jnp.zeros((chains, LANES), F32))

    def loss(i, acc):
        z = zt[i]
        soft = jnp.maximum(z, 0.0) + jnp.log1p(jnp.exp(-jnp.abs(z)))
        term = soft - label_row(i, z_rows) * z
        for q in range(z_rows // LANES):
            acc = acc + term[:, q * LANES:(q + 1) * LANES]
        return acc

    stages = {"g": grad_twin, "h": grad_own, "p": pair_sum, "c": chip_sum, "u": update,
              "m": gather, "o": logits_own, "t": logits_twin, "e": first_end, "l": add_loss}
    always = "ghpcuel"
    plan = PLAN

    def one_eval(t, carry):
        at = 0
        while at < len(plan):
            end = at
            while end < len(plan) and (plan[end][0] in always) == (plan[at][0] in always):
                end += 1

            def run(chunk=tuple(plan[at:end])):
                for op in chunk:
                    stages[op[0]](int(op[1:] or 0), t)

            if plan[at][0] in always:
                run()
            else:
                pl.when(t < LEAPS)(run)
            at = end
        return carry

    lax.fori_loop(0, LEAPS + 1, one_eval, 0)

    acc = lsum[...]
    for j in range(nb):
        for h in range(2):
            own = tf[j, 0, h] * tf[j, 0, h] * (1.0 / (2.0 * PRIOR_VAR)) + 0.5 * (pf[j, 0, h] * pf[j, 0, h])
            twin = tf[j, 1, h] * tf[j, 1, h] * (1.0 / (2.0 * PRIOR_VAR)) + 0.5 * (pf[j, 1, h] * pf[j, 1, h])
            acc = acc + jnp.concatenate([jnp.where(h == y, own, 0.0), jnp.where(h == x, twin, 0.0)], axis=0)
    row = jnp.sum(acc.T, axis=0, keepdims=True)
    ebuf[me] = jnp.broadcast_to(row, (8, chains))
    sends = []
    for n, dev in enumerate(others):
        cp = remote(ebuf.at[me], ebuf.at[me], en_s.at[n], en_r.at[n], dev)
        cp.start()
        sends.append(cp)

    for cp in sends:
        cp.wait()
    total = ebuf[0]
    for n in range(1, 8):
        total = total + ebuf[n]
    en_out[...] = total[0:1]

    def put(n, k):
        cc = (c, co)[k]
        return pltpu.make_async_copy(gb.at[:, n, cc], (th_out, mo_out)[n].at[:, cc], io_sem.at[2 * k + n])

    def swap(n):
        return remote(gb.at[:, n, c], gb.at[:, n, c], fd_s.at[n], fd_r.at[n], core)

    for n in range(2):
        state = (tf, pf)[n]
        for j in range(nb):
            last_copy(n, j).wait()
            gb[j, n, c, x] = jnp.concatenate([state[j, 0, y], state[j, 1, x]], axis=0).T
            gb[j, n, c, xo] = jnp.concatenate([xt[n, j], state[j, 1, xo]], axis=0).T
        swap(n).start()
        put(n, 0).start()
    for n in range(2):
        swap(n).wait()
        put(n, 1).start()
    for n in range(2):
        put(n, 0).wait()
        put(n, 1).wait()


def solution(mesh):
    chain_spec = P("feat", "parts")

    def local_run(x_local, labels, theta_init, mom_init, step_size):
        n_local, feats_half = x_local.shape
        rows = n_local // 2
        chains = theta_init.shape[1]
        nb = feats_half // (4 * LANES)
        z_rows = min(4 * LANES, rows)
        n_x = 2 * nb
        tiles = (nb, 2, 2, LANES, chains)
        vm = pl.BlockSpec(memory_space=pltpu.VMEM)
        dma = pltpu.SemaphoreType.DMA
        far = pl.BlockSpec(memory_space=pl.ANY)
        th, mo, en = pl.pallas_call(
            hmc_kernel,
            out_shape=(jax.ShapeDtypeStruct(tiles, F32), jax.ShapeDtypeStruct(tiles, F32),
                       jax.ShapeDtypeStruct((1, chains), F32)),
            in_specs=[far, vm, far, far, vm],
            out_specs=(far, far, vm),
            scratch_shapes=[
                pltpu.VMEM((3 * nb, rows, 4 * LANES), BF16),
                pltpu.VMEM((rows // z_rows, chains, z_rows), F32),
                pltpu.VMEM((chains, rows), BF16),
                pltpu.VMEM((nb, 2, 2, 2, chains, LANES), F32),
                pltpu.VMEM((nb, 2, 2, chains, LANES), F32),
                pltpu.VMEM((nb, 2, 2, chains // 2, LANES), F32),
                pltpu.VMEM((nb, 2, 2, chains // 2, LANES), F32),
                pltpu.VMEM((nb, 2, 2, chains // 2, LANES), F32),
                pltpu.VMEM((nb, 2, 2, 2, 2, chains // 2, LANES), BF16),
                pltpu.VMEM((nb, 2, 2, chains // 2, LANES), F32),
                pltpu.VMEM((nb, 2, 2, chains // 2, LANES), F32),
                pltpu.VMEM((2, nb, chains // 2, LANES), F32),
                pltpu.VMEM((chains, LANES), F32),
                pltpu.VMEM((chains, LANES), F32),
                pltpu.VMEM((8, 8, chains), F32),
                dma((n_x,)), dma((4,)), dma((n_x,)), dma((n_x,)), dma((2,)), dma((2,)), dma((nb,)), dma((nb,)),
                dma((nb, 2)), dma((nb, 2)), dma((nb, 2)), dma((nb, 2)),
                dma((nb, 2)), dma((nb, 2)), dma((nb,)), dma((nb,)),
                dma((2, nb)), dma((2, nb)), dma((2,)), dma((2,)), dma((7,)), dma((7,)),
            ],
            compiler_params=pltpu.CompilerParams(collective_id=0, has_side_effects=True,
                                                 vmem_limit_bytes=67043328),
        )(x_local, labels[None, :], theta_init.reshape(tiles), mom_init.reshape(tiles),
          step_size[None, :])
        return th.reshape(theta_init.shape), mo.reshape(theta_init.shape), en.reshape(chains)

    return jax.shard_map(local_run, mesh=mesh,
                         in_specs=(P("data", "feat"), P("data"), chain_spec, chain_spec, P("parts")),
                         out_specs=(chain_spec, chain_spec, P("parts")), check_vma=False)
```

```python
import functools

import jax
import jax.numpy as jnp
from jax import lax
from jax.experimental import pallas as pl
from jax.experimental.pallas import tpu as pltpu
from jax.sharding import PartitionSpec as P

LEAPS = 16
PRIOR_VAR = 4.0
MESH = pl.DeviceIdType.MESH
LANES = 128
PLAN = (
        "e0", "g0", "h0", "g1", "p0", "h1", "g2", "p1", "h2", "p2", "c0", "g3",
        "c1", "h3", "p3", "l0", "s0", "u0", "c2", "c3", "u1", "m0", "o0", "u2",
        "t0", "u3", "m1", "o1", "m2", "o2", "t1", "m3", "o3", "t2", "t3",
)
F32 = jnp.float32
BF16 = jnp.bfloat16


def contract_last(a, b):
    return lax.dot_general(a, b, (((1,), (1,)), ((), ())), preferred_element_type=F32)


def hmc_kernel(x_hbm, lab_ref, theta_ref, mom_ref, eps_ref,
               st_out, en_out,
               xa, zt, rt, gb, dd, r1, h2, r2, tb, tf, pf, xt, eb, lsum, ebuf,
               loc_sem, io_sem, xs_s, xs_r, in_s, in_r, sd_s, sd_r, ds_s, ds_r, r1_s, r1_r, r2_s, r2_r, a1_s, a1_r, ad_s, ad_r,
               fx_s, fx_r, fd_s, fd_r, en_s, en_r):
    nb = tb.shape[0]
    chains = zt.shape[1]
    n_zc, z_rows = zt.shape[0], zt.shape[2]
    rows = n_zc * z_rows
    wide = 4 * LANES
    strip = 2 * LANES
    n_x = 2 * nb
    part = lax.axis_index("parts")
    y = lax.axis_index("feat")
    d = lax.axis_index("data")
    x = d // 2
    c = d % 2
    xo, yo, co = 1 - x, 1 - y, 1 - c
    x_nbr = (part, y, 2 * xo + c)
    y_nbr = (part, yo, 2 * x + c)
    core = (part, y, 2 * x + co)
    pair = (x_nbr, y_nbr)
    half = chains // 2
    me = 4 * y + d

    def remote(src, dst, s_sem, r_sem, dev):
        return pltpu.make_async_remote_copy(src_ref=src, dst_ref=dst, send_sem=s_sem, recv_sem=r_sem,
                                            device_id=dev, device_id_type=MESH)

    others = []
    for dy in range(2):
        for dd_ in range(4):
            if dy or dd_:
                others.append((part, (y + dy) % 2, (d + dd_) % 4))

    barrier = pltpu.get_barrier_semaphore()
    for dev in others:
        pl.semaphore_signal(barrier, inc=1, device_id=dev, device_id_type=MESH)
    pl.semaphore_wait(barrier, 7)

    def strip_refs(u, here, at=0, n=rows):
        src = x_hbm.at[pl.ds(pl.multiple_of(here * rows + at, n), n), pl.ds(pl.multiple_of(u * strip, strip), strip)]
        return src, xa.at[u, at:at + n, pl.ds(pl.multiple_of(y * strip, strip), strip)]

    def x_copy(u):
        return remote(*strip_refs(u, yo), xs_s.at[u], xs_r.at[u], y_nbr)

    parts = 4

    def x_last(k):
        n = rows // parts
        sem = 1 if k == 0 else n_x + k - 1
        return remote(*strip_refs(1, yo, k * n, n), xs_s.at[sem], xs_r.at[sem], y_nbr)

    def x_local(u):
        return pltpu.make_async_copy(*strip_refs(u, y), loc_sem.at[u])

    def d2d_copy(j):
        return remote(gb.at[j, co], dd.at[j], ds_s.at[j], ds_r.at[j], core)

    def rs1_copy(j, k):
        src = (gb.at[j, c, :, xo, :half], gb.at[j, c, yo, :, half:])[k]
        return remote(src, r1.at[j, k], r1_s.at[j, k], r1_r.at[j, k], pair[k])

    def rs2_copy(j, k):
        return remote(h2.at[j, k], r2.at[j, k], r2_s.at[j, k], r2_r.at[j, k], pair[1 - k])

    def ag1_copy(j, k):
        ref = (tb.at[j, c, 0, :, x], tb.at[j, c, 1, y])[k]
        return remote(ref, ref, a1_s.at[j, k], a1_r.at[j, k], pair[k])

    def seed_copy(n):
        ref = (tb.at[:, c, :, y, x], tb.at[:, c, :, :, x])[n]
        return remote(ref, ref, sd_s.at[n], sd_r.at[n], pair[1 - n])

    def start_copy(n):
        ref = (tf, pf)[n].at[:, 0, y]
        return remote(ref, ref, in_s.at[n], in_r.at[n], y_nbr)

    def last_copy(n, j):
        return remote((tf, pf)[n].at[j, 0, y], xt.at[n, j], fx_s.at[n, j], fx_r.at[n, j], x_nbr)

    def agd_copy(j):
        return remote(tb.at[j, c], tb.at[j, c], ad_s.at[j], ad_r.at[j], core)

    ahead = 1

    def strip_at(i):
        return n_x - 2 - 2 * (i // 2) + i % 2

    staged = [pltpu.make_async_copy(ref.at[:, c], gb.at[:, n, c], io_sem.at[n])
              for n, ref in enumerate((theta_ref, mom_ref))]
    for cp in staged:
        cp.start()
    for i in range(ahead):
        x_copy(strip_at(i)).start()
    for i in range(n_x):
        x_local(strip_at(i)).start()
    eb[...] = jnp.broadcast_to(eps_ref[...], (LANES, chains)).T
    for cp in staged:
        cp.wait()
    for j in range(nb):
        for xx in range(2):
            tf[j, 1, xx] = gb[j, 0, c, xx].T[half:]
            pf[j, 1, xx] = gb[j, 1, c, xx].T[half:]
        tf[j, 0, y] = gb[j, 0, c, x].T[:half]
        pf[j, 0, y] = gb[j, 1, c, x].T[:half]
        tb[j, c, 0, y, x] = tf[j, 0, y].astype(BF16)
        tb[j, c, 1, y, x] = tf[j, 1, x].astype(BF16)
    seed_copy(0).start()

    @pl.loop(ahead, n_x - 1)
    def _(i):
        x_copy(strip_at(i)).start()

    for k in range(parts):
        x_last(k).start()

    for n in range(2):
        start_copy(n).start()

    def gather_mid(j):
        for k in range(2):
            ag1_copy(j, k).wait()
        agd_copy(j).start()

    def gather_end(j):
        agd_copy(j).wait()

    for n in range(2):
        seed_copy(n).wait()
        if n == 0:
            seed_copy(1).start()
    for j in range(nb):
        agd_copy(j).start()
    for j in range(nb):
        gather_end(j)

    def lhs_of(j, cc):
        return jnp.concatenate([jnp.concatenate([tb[j, cc, k, h, xx] for h in range(2) for xx in range(2)], axis=1)
                                for k in range(2)], axis=0)

    def label_row(i, n):
        return lab_ref[:, pl.ds(pl.multiple_of(y * rows + i * n, n), n)].astype(F32)

    def residual(i, z):
        lab = label_row(i, z_rows)
        rt[:, pl.ds(pl.multiple_of(i * z_rows, z_rows), z_rows)] = (lab - jax.nn.sigmoid(z)).astype(BF16)

    def piece(q):
        return slice(q * z_rows, (q + 1) * z_rows)

    def logits_plain(j, cc, first):
        left = lhs_of(j, cc)
        for q in range(n_zc):
            new = contract_last(left, xa[2 * j + cc, piece(q)])
            zt[q] = new if first is True else jnp.where(first, 0.0, zt[q]) + new

    def logits_flip(j, cc, end):
        left = lhs_of(j, cc)
        for q in range(n_zc):
            z = zt[q] + jnp.dot(left, xa[nb + 2 * j + cc, piece(q)], preferred_element_type=F32)
            zt[q] = z
            if end:
                residual(q, z)

    @pl.loop(0, n_x - 1)
    def _(i):
        u = strip_at(i)
        j, cc = u // 2, u % 2
        x_local(u).wait()
        x_copy(u).wait_recv()
        logits_plain(j, cc, i == 0)

        @pl.when(j > 0)
        def _():
            for q in range(n_zc):
                xa[nb + u, piece(q)] = xa[u, piece(q)].T

    x_local(1).wait()
    left = lhs_of(0, 1)
    for k in range(parts):
        x_last(k).wait_recv()
        for q in range(k * n_zc // parts, (k + 1) * n_zc // parts):
            residual(q, zt[q] + contract_last(left, xa[1, piece(q)]))

    @pl.loop(0, n_x - 1)
    def _(i):
        x_copy(strip_at(i)).wait_send()

    for k in range(parts):
        x_last(k).wait_send()


    def grad_half(j, p):
        if j < nb - 1:
            out = jnp.dot(rt[...], xa[2 * j + p], preferred_element_type=F32)
        else:
            out = contract_last(rt[:, piece(0)], xa[nb + 2 * j + p, piece(0)])
            for q in range(1, n_zc):
                out = out + contract_last(rt[:, piece(q)], xa[nb + 2 * j + p, piece(q)])
        for q in range(4):
            gb[j, p, q // 2, q % 2] = out[:, q * LANES:(q + 1) * LANES]

    def grad_twin(j, t):
        grad_half(j, co)
        d2d_copy(j).start()

    def grad_own(j, t):
        grad_half(j, c)

    def pair_sum(j, t):
        d2d_copy(j).wait()
        gb[j, c] += dd[j]
        for k in range(2):
            rs1_copy(j, k).start()

    def chip_sum(j, t):
        for k in range(2):
            rs1_copy(j, k).wait()
        h2[j, 0] = gb[j, c, :, x, :half] + r1[j, 0]
        h2[j, 1] = gb[j, c, y, :, half:] + r1[j, 1]
        for k in range(2):
            rs2_copy(j, k).start()

    def update(j, t):
        for k in range(2):
            rs2_copy(j, k).wait()
        pos = tf[j]
        eps = eb[...].reshape(2, 1, half, LANES)
        ends = jnp.logical_or(t == 0, t == LEAPS)
        mom = pf[j] + eps * jnp.where(ends, 0.5, 1.0) * ((h2[j] + r2[j]) - pos / PRIOR_VAR)
        pf[j] = mom

        @pl.when(t < LEAPS)
        def _():
            new = pos + eps * mom
            tf[j] = new
            low = new.astype(BF16)
            tb[j, c, 0, :, x] = low[0]
            tb[j, c, 1, y] = low[1]
            for k in range(2):
                ag1_copy(j, k).start()

        @pl.when(t == LEAPS)
        def _():
            last_copy(1, j).start()

    def logits_own(j, t):
        if j == 0:
            logits_plain(j, c, True)
        else:
            logits_flip(j, c, False)

    def logits_twin(j, t):
        gather_end(j)
        if j == 0:
            logits_plain(j, co, False)
        else:
            logits_flip(j, co, j == nb - 1)

    def gather(j, t):
        gather_mid(j)

    def start_end(j, t):
        @pl.when(t == 0)
        def _():
            for n in range(2):
                start_copy(n).wait()

    def first_end(j, t):
        @pl.when(t == LEAPS)
        def _():
            for i in range(nb):
                last_copy(0, i).start()

    def add_loss(j, t):
        @pl.when(t == LEAPS)
        def _():
            lsum[...] = lax.fori_loop(0, n_zc, loss, jnp.zeros((chains, LANES), F32))

    def loss(i, acc):
        z = zt[i]
        soft = jnp.maximum(z, 0.0) + jnp.log1p(jnp.exp(-jnp.abs(z)))
        term = soft - label_row(i, z_rows) * z
        for q in range(z_rows // LANES):
            acc = acc + term[:, q * LANES:(q + 1) * LANES]
        return acc

    stages = {"g": grad_twin, "h": grad_own, "p": pair_sum, "c": chip_sum, "u": update,
              "m": gather, "o": logits_own, "t": logits_twin, "e": first_end, "l": add_loss, "s": start_end}
    always = set("ghpcuels")
    plan = PLAN

    def one_eval(t, carry):
        at = 0
        while at < len(plan):
            end = at
            while end < len(plan) and (plan[end][0] in always) == (plan[at][0] in always):
                end += 1

            def run(chunk=tuple(plan[at:end])):
                for op in chunk:
                    stages[op[0]](int(op[1:] or 0), t)

            if plan[at][0] in always:
                run()
            else:
                pl.when(t < LEAPS)(run)
            at = end
        return carry

    lax.fori_loop(0, LEAPS + 1, one_eval, 0)

    acc = lsum[...]
    for j in range(nb):
        for h in range(2):
            own = tf[j, 0, h] * tf[j, 0, h] * (1.0 / (2.0 * PRIOR_VAR)) + 0.5 * (pf[j, 0, h] * pf[j, 0, h])
            twin = tf[j, 1, h] * tf[j, 1, h] * (1.0 / (2.0 * PRIOR_VAR)) + 0.5 * (pf[j, 1, h] * pf[j, 1, h])
            acc = acc + jnp.concatenate([jnp.where(h == y, own, 0.0), jnp.where(h == x, twin, 0.0)], axis=0)
    row = jnp.sum(acc.T, axis=0, keepdims=True)
    ebuf[me] = jnp.broadcast_to(row, (8, chains))
    sends = []
    for n, dev in enumerate(others):
        cp = remote(ebuf.at[me], ebuf.at[me], en_s.at[n], en_r.at[n], dev)
        cp.start()
        sends.append(cp)

    for cp in sends:
        cp.wait()
    total = ebuf[0]
    for n in range(1, 8):
        total = total + ebuf[n]
    en_out[...] = total[0:1]

    def put(n, k):
        cc = (c, co)[k]
        return pltpu.make_async_copy(gb.at[:, n, cc], st_out.at[n, :, cc], io_sem.at[2 * k + n])

    def swap(n):
        return remote(gb.at[:, n, c], gb.at[:, n, c], fd_s.at[n], fd_r.at[n], core)

    for n in range(2):
        state = (tf, pf)[n]
        for j in range(nb):
            last_copy(n, j).wait()
            gb[j, n, c, x] = jnp.concatenate([state[j, 0, y], state[j, 1, x]], axis=0).T
            gb[j, n, c, xo] = jnp.concatenate([xt[n, j], state[j, 1, xo]], axis=0).T
        swap(n).start()
        put(n, 0).start()
    for n in range(2):
        swap(n).wait()
        put(n, 1).start()
    for n in range(2):
        put(n, 0).wait()
        put(n, 1).wait()


def solution(mesh):
    chain_spec = P("feat", "parts")

    def local_run(x_local, labels, theta_init, mom_init, step_size):
        n_local, feats_half = x_local.shape
        rows = n_local // 2
        chains = theta_init.shape[1]
        nb = feats_half // (4 * LANES)
        z_rows = min(4 * LANES, rows)
        n_x = 2 * nb
        tiles = (nb, 2, 2, LANES, chains)
        vm = pl.BlockSpec(memory_space=pltpu.VMEM)
        dma = pltpu.SemaphoreType.DMA
        far = pl.BlockSpec(memory_space=pl.ANY)
        state, en = pl.pallas_call(
            hmc_kernel,
            out_shape=(jax.ShapeDtypeStruct((2,) + tiles, F32), jax.ShapeDtypeStruct((1, chains), F32)),
            in_specs=[far, vm, far, far, vm],
            out_specs=(far, vm),
            scratch_shapes=[
                pltpu.VMEM((3 * nb, rows, 4 * LANES), BF16),
                pltpu.VMEM((rows // z_rows, chains, z_rows), F32),
                pltpu.VMEM((chains, rows), BF16),
                pltpu.VMEM((nb, 2, 2, 2, chains, LANES), F32),
                pltpu.VMEM((nb, 2, 2, chains, LANES), F32),
                pltpu.VMEM((nb, 2, 2, chains // 2, LANES), F32),
                pltpu.VMEM((nb, 2, 2, chains // 2, LANES), F32),
                pltpu.VMEM((nb, 2, 2, chains // 2, LANES), F32),
                pltpu.VMEM((nb, 2, 2, 2, 2, chains // 2, LANES), BF16),
                pltpu.VMEM((nb, 2, 2, chains // 2, LANES), F32),
                pltpu.VMEM((nb, 2, 2, chains // 2, LANES), F32),
                pltpu.VMEM((2, nb, chains // 2, LANES), F32),
                pltpu.VMEM((chains, LANES), F32),
                pltpu.VMEM((chains, LANES), F32),
                pltpu.VMEM((8, 8, chains), F32),
                dma((n_x,)), dma((4,)), dma((n_x + 3,)), dma((n_x + 3,)), dma((2,)), dma((2,)), dma((2,)), dma((2,)), dma((nb,)), dma((nb,)),
                dma((nb, 2)), dma((nb, 2)), dma((nb, 2)), dma((nb, 2)),
                dma((nb, 2)), dma((nb, 2)), dma((nb,)), dma((nb,)),
                dma((2, nb)), dma((2, nb)), dma((2,)), dma((2,)), dma((7,)), dma((7,)),
            ],
            compiler_params=pltpu.CompilerParams(collective_id=0, has_side_effects=True,
                                                 vmem_limit_bytes=67043328),
        )(x_local, labels[None, :], theta_init.reshape(tiles), mom_init.reshape(tiles),
          step_size[None, :])
        return state[0].reshape(theta_init.shape), state[1].reshape(theta_init.shape), en.reshape(chains)

    return jax.shard_map(local_run, mesh=mesh,
                         in_specs=(P("data", "feat"), P("data"), chain_spec, chain_spec, P("parts")),
                         out_specs=(chain_spec, chain_spec, P("parts")), check_vma=False)
```

```python
import functools

import jax
import jax.numpy as jnp
from jax import lax
from jax.experimental import pallas as pl
from jax.experimental.pallas import tpu as pltpu
from jax.sharding import PartitionSpec as P

LEAPS = 16
PRIOR_VAR = 4.0
MESH = pl.DeviceIdType.MESH
LANES = 128
PLAN = (
        "e0", "g1", "h0", "p0", "h1", "g2", "p1", "h2", "p2", "c0", "g3", "c1",
        "h3", "p3", "l0", "s0", "u0", "c2", "c3", "u1", "m0", "o0", "u2", "t0",
        "u3", "m1", "o1", "m2", "o2", "t1", "m3", "o3", "t2", "t3", "n0",
)
F32 = jnp.float32
BF16 = jnp.bfloat16


def contract_last(a, b):
    return lax.dot_general(a, b, (((1,), (1,)), ((), ())), preferred_element_type=F32)


def hmc_kernel(x_hbm, lab_ref, theta_ref, mom_ref, eps_ref,
               st_out, en_out,
               xa, zt, rt, gb, dd, r1, h2, r2, tb, tf, pf, xt, eb, lsum, ebuf,
               loc_sem, io_sem, xs_s, xs_r, in_s, in_r, sd_s, sd_r, ds_s, ds_r, r1_s, r1_r, r2_s, r2_r, a1_s, a1_r, ad_s, ad_r,
               fx_s, fx_r, fd_s, fd_r, en_s, en_r):
    nb = tb.shape[0]
    chains = zt.shape[1]
    n_zc, z_rows = zt.shape[0], zt.shape[2]
    rows = n_zc * z_rows
    wide = 4 * LANES
    strip = 2 * LANES
    n_x = 2 * nb
    part = lax.axis_index("parts")
    y = lax.axis_index("feat")
    d = lax.axis_index("data")
    x = d // 2
    c = d % 2
    xo, yo, co = 1 - x, 1 - y, 1 - c
    x_nbr = (part, y, 2 * xo + c)
    y_nbr = (part, yo, 2 * x + c)
    core = (part, y, 2 * x + co)
    pair = (x_nbr, y_nbr)
    half = chains // 2
    me = 4 * y + d

    def remote(src, dst, s_sem, r_sem, dev):
        return pltpu.make_async_remote_copy(src_ref=src, dst_ref=dst, send_sem=s_sem, recv_sem=r_sem,
                                            device_id=dev, device_id_type=MESH)

    others = []
    for dy in range(2):
        for dd_ in range(4):
            if dy or dd_:
                others.append((part, (y + dy) % 2, (d + dd_) % 4))

    barrier = pltpu.get_barrier_semaphore()
    for dev in others:
        pl.semaphore_signal(barrier, inc=1, device_id=dev, device_id_type=MESH)
    pl.semaphore_wait(barrier, 7)

    def strip_refs(u, here, at=0, n=rows):
        src = x_hbm.at[pl.ds(pl.multiple_of(here * rows + at, n), n), pl.ds(pl.multiple_of(u * strip, strip), strip)]
        return src, xa.at[u, at:at + n, pl.ds(pl.multiple_of(y * strip, strip), strip)]

    def x_copy(u):
        return remote(*strip_refs(u, yo), xs_s.at[u], xs_r.at[u], y_nbr)

    parts = 4

    def x_last(k):
        n = rows // parts
        sem = 1 if k == 0 else n_x + k - 1
        return remote(*strip_refs(1, yo, k * n, n), xs_s.at[sem], xs_r.at[sem], y_nbr)

    def x_local(u):
        return pltpu.make_async_copy(*strip_refs(u, y), loc_sem.at[u])

    def d2d_copy(j):
        return remote(gb.at[j, co], dd.at[j], ds_s.at[j], ds_r.at[j], core)

    def rs1_copy(j, k):
        src = (gb.at[j, c, :, xo, :half], gb.at[j, c, yo, :, half:])[k]
        return remote(src, r1.at[j, k], r1_s.at[j, k], r1_r.at[j, k], pair[k])

    def rs2_copy(j, k):
        return remote(h2.at[j, k], r2.at[j, k], r2_s.at[j, k], r2_r.at[j, k], pair[1 - k])

    def ag1_copy(j, k):
        ref = (tb.at[j, c, 0, :, x], tb.at[j, c, 1, y])[k]
        return remote(ref, ref, a1_s.at[j, k], a1_r.at[j, k], pair[k])

    def seed_copy(n):
        ref = (tb.at[:, c, :, y, x], tb.at[:, c, :, :, x])[n]
        return remote(ref, ref, sd_s.at[n], sd_r.at[n], pair[1 - n])

    def start_copy(n):
        ref = (tf, pf)[n].at[:, 0, y]
        return remote(ref, ref, in_s.at[n], in_r.at[n], y_nbr)

    def last_copy(n, j):
        return remote((tf, pf)[n].at[j, 0, y], xt.at[n, j], fx_s.at[n, j], fx_r.at[n, j], x_nbr)

    def agd_copy(j):
        return remote(tb.at[j, c], tb.at[j, c], ad_s.at[j], ad_r.at[j], core)

    ahead = 1

    def strip_at(i):
        return n_x - 2 - 2 * (i // 2) + i % 2

    staged = [pltpu.make_async_copy(ref.at[:, c], gb.at[:, n, c], io_sem.at[n])
              for n, ref in enumerate((theta_ref, mom_ref))]
    for cp in staged:
        cp.start()
    for i in range(ahead):
        x_copy(strip_at(i)).start()
    for i in range(n_x):
        x_local(strip_at(i)).start()
    eb[...] = jnp.broadcast_to(eps_ref[...], (LANES, chains)).T
    for cp in staged:
        cp.wait()
    for j in range(nb):
        for xx in range(2):
            tf[j, 1, xx] = gb[j, 0, c, xx].T[half:]
            pf[j, 1, xx] = gb[j, 1, c, xx].T[half:]
        tf[j, 0, y] = gb[j, 0, c, x].T[:half]
        pf[j, 0, y] = gb[j, 1, c, x].T[:half]
        tb[j, c, 0, y, x] = tf[j, 0, y].astype(BF16)
        tb[j, c, 1, y, x] = tf[j, 1, x].astype(BF16)
    seed_copy(0).start()

    @pl.loop(ahead, n_x - 1)
    def _(i):
        x_copy(strip_at(i)).start()

    for k in range(parts):
        x_last(k).start()

    for n in range(2):
        start_copy(n).start()

    def gather_mid(j):
        for k in range(2):
            ag1_copy(j, k).wait()
        agd_copy(j).start()

    def gather_end(j):
        agd_copy(j).wait()

    for n in range(2):
        seed_copy(n).wait()
        if n == 0:
            seed_copy(1).start()
    for j in range(nb):
        agd_copy(j).start()
    for j in range(nb):
        gather_end(j)

    def lhs_of(j, cc):
        return jnp.concatenate([jnp.concatenate([tb[j, cc, k, h, xx] for h in range(2) for xx in range(2)], axis=1)
                                for k in range(2)], axis=0)

    def label_row(i, n):
        return lab_ref[:, pl.ds(pl.multiple_of(y * rows + i * n, n), n)].astype(F32)

    def residual(i, z):
        lab = label_row(i, z_rows)
        rt[:, pl.ds(pl.multiple_of(i * z_rows, z_rows), z_rows)] = (lab - jax.nn.sigmoid(z)).astype(BF16)

    def piece(q):
        return slice(q * z_rows, (q + 1) * z_rows)

    def logits_plain(j, cc, first):
        left = lhs_of(j, cc)
        for q in range(n_zc):
            new = contract_last(left, xa[2 * j + cc, piece(q)])
            zt[q] = new if first is True else jnp.where(first, 0.0, zt[q]) + new

    def logits_flip(j, cc, end):
        left = lhs_of(j, cc)
        for q in range(n_zc):
            z = zt[q] + jnp.dot(left, xa[nb + 2 * j + cc, piece(q)], preferred_element_type=F32)
            zt[q] = z
            if end:
                residual(q, z)

    @pl.loop(0, n_x - 1)
    def _(i):
        u = strip_at(i)
        j, cc = u // 2, u % 2
        x_local(u).wait()
        x_copy(u).wait_recv()
        logits_plain(j, cc, i == 0)

        @pl.when(j > 0)
        def _():
            for q in range(n_zc):
                xa[nb + u, piece(q)] = xa[u, piece(q)].T

    x_local(1).wait()
    left = lhs_of(0, 1)
    for k in range(parts):
        x_last(k).wait_recv()
        for q in range(k * n_zc // parts, (k + 1) * n_zc // parts):
            residual(q, zt[q] + contract_last(left, xa[1, piece(q)]))

    @pl.loop(0, n_x - 1)
    def _(i):
        x_copy(strip_at(i)).wait_send()

    for k in range(parts):
        x_last(k).wait_send()


    def grad_half(j, p):
        if j < nb - 1:
            out = jnp.dot(rt[...], xa[2 * j + p], preferred_element_type=F32)
        else:
            out = contract_last(rt[:, piece(0)], xa[nb + 2 * j + p, piece(0)])
            for q in range(1, n_zc):
                out = out + contract_last(rt[:, piece(q)], xa[nb + 2 * j + p, piece(q)])
        for q in range(4):
            gb[j, p, q // 2, q % 2] = out[:, q * LANES:(q + 1) * LANES]

    def grad_twin(j, t):
        grad_half(j, co)
        d2d_copy(j).start()

    def grad_own(j, t):
        grad_half(j, c)

    def pair_sum(j, t):
        d2d_copy(j).wait()
        gb[j, c] += dd[j]
        for k in range(2):
            rs1_copy(j, k).start()

    def chip_sum(j, t):
        for k in range(2):
            rs1_copy(j, k).wait()
        h2[j, 0] = gb[j, c, :, x, :half] + r1[j, 0]
        h2[j, 1] = gb[j, c, y, :, half:] + r1[j, 1]
        for k in range(2):
            rs2_copy(j, k).start()

    def update(j, t):
        for k in range(2):
            rs2_copy(j, k).wait()
        pos = tf[j]
        eps = eb[...].reshape(2, 1, half, LANES)
        ends = jnp.logical_or(t == 0, t == LEAPS)
        mom = pf[j] + eps * jnp.where(ends, 0.5, 1.0) * ((h2[j] + r2[j]) - pos / PRIOR_VAR)
        pf[j] = mom

        @pl.when(t < LEAPS)
        def _():
            new = pos + eps * mom
            tf[j] = new
            low = new.astype(BF16)
            tb[j, c, 0, :, x] = low[0]
            tb[j, c, 1, y] = low[1]
            for k in range(2):
                ag1_copy(j, k).start()

        @pl.when(t == LEAPS)
        def _():
            last_copy(1, j).start()

    def logits_own(j, t):
        if j == 0:
            logits_plain(j, c, True)
        else:
            logits_flip(j, c, False)

    def logits_twin(j, t):
        gather_end(j)
        if j == 0:
            logits_plain(j, co, False)
        else:
            logits_flip(j, co, j == nb - 1)

    def gather(j, t):
        gather_mid(j)

    def start_end(j, t):
        @pl.when(t == 0)
        def _():
            for n in range(2):
                start_copy(n).wait()

    def first_end(j, t):
        @pl.when(t == LEAPS)
        def _():
            for i in range(nb):
                last_copy(0, i).start()

    def add_loss(j, t):
        @pl.when(t == LEAPS)
        def _():
            lsum[...] = lax.fori_loop(0, n_zc, loss, jnp.zeros((chains, LANES), F32))

    def loss(i, acc):
        z = zt[i]
        soft = jnp.maximum(z, 0.0) + jnp.log1p(jnp.exp(-jnp.abs(z)))
        term = soft - label_row(i, z_rows) * z
        for q in range(z_rows // LANES):
            acc = acc + term[:, q * LANES:(q + 1) * LANES]
        return acc

    stages = {"g": grad_twin, "h": grad_own, "p": pair_sum, "c": chip_sum, "u": update,
              "m": gather, "o": logits_own, "t": logits_twin, "n": grad_twin, "e": first_end, "l": add_loss, "s": start_end}
    always = set("ghpcuels")
    plan = PLAN

    def one_eval(t, carry):
        at = 0
        while at < len(plan):
            end = at
            while end < len(plan) and (plan[end][0] in always) == (plan[at][0] in always):
                end += 1

            def run(chunk=tuple(plan[at:end])):
                for op in chunk:
                    stages[op[0]](int(op[1:] or 0), t)

            if plan[at][0] in always:
                run()
            else:
                pl.when(t < LEAPS)(run)
            at = end
        return carry

    grad_twin(0, 0)
    lax.fori_loop(0, LEAPS + 1, one_eval, 0)

    acc = lsum[...]
    for j in range(nb):
        for h in range(2):
            own = tf[j, 0, h] * tf[j, 0, h] * (1.0 / (2.0 * PRIOR_VAR)) + 0.5 * (pf[j, 0, h] * pf[j, 0, h])
            twin = tf[j, 1, h] * tf[j, 1, h] * (1.0 / (2.0 * PRIOR_VAR)) + 0.5 * (pf[j, 1, h] * pf[j, 1, h])
            acc = acc + jnp.concatenate([jnp.where(h == y, own, 0.0), jnp.where(h == x, twin, 0.0)], axis=0)
    row = jnp.sum(acc.T, axis=0, keepdims=True)
    ebuf[me] = jnp.broadcast_to(row, (8, chains))
    sends = []
    for n, dev in enumerate(others):
        cp = remote(ebuf.at[me], ebuf.at[me], en_s.at[n], en_r.at[n], dev)
        cp.start()
        sends.append(cp)

    for cp in sends:
        cp.wait()
    total = ebuf[0]
    for n in range(1, 8):
        total = total + ebuf[n]
    en_out[...] = total[0:1]

    def put(n, k):
        cc = (c, co)[k]
        return pltpu.make_async_copy(gb.at[:, n, cc], st_out.at[n, :, cc], io_sem.at[2 * k + n])

    def swap(n):
        return remote(gb.at[:, n, c], gb.at[:, n, c], fd_s.at[n], fd_r.at[n], core)

    for n in range(2):
        state = (tf, pf)[n]
        for j in range(nb):
            last_copy(n, j).wait()
            gb[j, n, c, x] = jnp.concatenate([state[j, 0, y], state[j, 1, x]], axis=0).T
            gb[j, n, c, xo] = jnp.concatenate([xt[n, j], state[j, 1, xo]], axis=0).T
        swap(n).start()
        put(n, 0).start()
    for n in range(2):
        swap(n).wait()
        put(n, 1).start()
    for n in range(2):
        put(n, 0).wait()
        put(n, 1).wait()


def solution(mesh):
    chain_spec = P("feat", "parts")

    def local_run(x_local, labels, theta_init, mom_init, step_size):
        n_local, feats_half = x_local.shape
        rows = n_local // 2
        chains = theta_init.shape[1]
        nb = feats_half // (4 * LANES)
        z_rows = min(4 * LANES, rows)
        n_x = 2 * nb
        tiles = (nb, 2, 2, LANES, chains)
        vm = pl.BlockSpec(memory_space=pltpu.VMEM)
        dma = pltpu.SemaphoreType.DMA
        far = pl.BlockSpec(memory_space=pl.ANY)
        state, en = pl.pallas_call(
            hmc_kernel,
            out_shape=(jax.ShapeDtypeStruct((2,) + tiles, F32), jax.ShapeDtypeStruct((1, chains), F32)),
            in_specs=[far, vm, far, far, vm],
            out_specs=(far, vm),
            scratch_shapes=[
                pltpu.VMEM((3 * nb, rows, 4 * LANES), BF16),
                pltpu.VMEM((rows // z_rows, chains, z_rows), F32),
                pltpu.VMEM((chains, rows), BF16),
                pltpu.VMEM((nb, 2, 2, 2, chains, LANES), F32),
                pltpu.VMEM((nb, 2, 2, chains, LANES), F32),
                pltpu.VMEM((nb, 2, 2, chains // 2, LANES), F32),
                pltpu.VMEM((nb, 2, 2, chains // 2, LANES), F32),
                pltpu.VMEM((nb, 2, 2, chains // 2, LANES), F32),
                pltpu.VMEM((nb, 2, 2, 2, 2, chains // 2, LANES), BF16),
                pltpu.VMEM((nb, 2, 2, chains // 2, LANES), F32),
                pltpu.VMEM((nb, 2, 2, chains // 2, LANES), F32),
                pltpu.VMEM((2, nb, chains // 2, LANES), F32),
                pltpu.VMEM((chains, LANES), F32),
                pltpu.VMEM((chains, LANES), F32),
                pltpu.VMEM((8, 8, chains), F32),
                dma((n_x,)), dma((4,)), dma((n_x + 3,)), dma((n_x + 3,)), dma((2,)), dma((2,)), dma((2,)), dma((2,)), dma((nb,)), dma((nb,)),
                dma((nb, 2)), dma((nb, 2)), dma((nb, 2)), dma((nb, 2)),
                dma((nb, 2)), dma((nb, 2)), dma((nb,)), dma((nb,)),
                dma((2, nb)), dma((2, nb)), dma((2,)), dma((2,)), dma((7,)), dma((7,)),
            ],
            compiler_params=pltpu.CompilerParams(collective_id=0, has_side_effects=True,
                                                 vmem_limit_bytes=67043328),
        )(x_local, labels[None, :], theta_init.reshape(tiles), mom_init.reshape(tiles),
          step_size[None, :])
        return state[0].reshape(theta_init.shape), state[1].reshape(theta_init.shape), en.reshape(chains)

    return jax.shard_map(local_run, mesh=mesh,
                         in_specs=(P("data", "feat"), P("data"), chain_spec, chain_spec, P("parts")),
                         out_specs=(chain_spec, chain_spec, P("parts")), check_vma=False)
```
